32 devices in a mesh: dp: 4 (over y, core), seq: 8 (over z, x).
Axes of the slice: x: 2, y: 2, z: 4, core: 2. Of those that a mesh axis runs over, the one named last changes fastest.
Arguments:
- head_inputs: bfloat16 [4, 3072, 1024], P('dp', 'seq'), may hold values from -6 to 6
- gate_inputs: bfloat16 [4, 3072, 1024], P('dp', 'seq'), may hold values from -6 to 6
- state_proj: bfloat16 [4, 3072, 256], P('dp', 'seq'), may hold values from -2 to 2
- time_steps: float32 [4, 3072, 16], P('dp', 'seq'), may hold values from -4.7 to 4.7
- token_ids: int32 [4, 3072], P('dp', 'seq'), may hold values from 0 to 50279, as said below
- token_counts: int32 [4], replicated, may hold values from 1536 to 3072
- teacher_out: bfloat16 [4, 3072, 1024], P('dp', 'seq'), may hold values from -6 to 6
- out_weight: float32 [1024, 1024], P(('dp', 'seq')), may hold values from -0.1875 to 0.1875
- decay_log: float32 [16], replicated, may hold values from -6.5 to 1
- step_bias: float32 [16], replicated, may hold values from -5 to -3
- skip_gain: float32 [16], replicated, may hold values from 0.5 to 1.5
- norm_gain: float32 [1024], replicated, may hold values from 0.5 to 1.5
Outputs:
- losses: float32 [2], replicated
- new_weight: float32 [1024, 1024], P(('dp', 'seq'))
- new_decay: float32 [16], replicated
- new_bias: float32 [16], replicated
- new_skip: float32 [16], replicated
- new_gain: float32 [1024], replicated
The draws below stay inside these ranges and needn't reach their ends.
Inputs may be any that keep to these rules, and one draw needn't show every extreme that they name: `token_ids`: in each sequence exactly one position, never the first, holds id 0.
All inputs are finite; a program needn't handle non-finite values.
Results may differ from the reference program's by a relative error of at most 0.0003.
Values may be sent and summed in bfloat16 or wider, within the bound.
A program may use at most 192 MiB of HBM per device.

```python
import jax
import jax.numpy as jnp
from jax import lax

D = 1024
N = 128
VOCAB = 50280
H = 16
STEPS = 2
TOK_DEV = 384
SEQS = 4
LENGTH = 3072
DI = 1024
N_SEQ = 8


def draw_time_steps(key, part):
    noise_key, shift_key = jax.random.split(key)
    blocks = LENGTH // TOK_DEV
    offset = jax.random.uniform(shift_key, (SEQS, blocks, 1, H), jnp.float32, -0.7, 0.7)
    jitter = jnp.clip(jax.random.normal(noise_key, (SEQS, blocks, TOK_DEV, H), jnp.float32), -4.0, 4.0)
    return (jitter + offset).reshape(SEQS, LENGTH, H)


def draw_decay_log(key, part):
    pick_key, strong_key, weak_key = jax.random.split(key, 3)
    strong = jax.random.randint(pick_key, (H,), 0, 2) > 0
    slow_rate = jax.random.uniform(strong_key, (H,), jnp.float32, -6.5, -5.5)
    quick_rate = jax.random.uniform(weak_key, (H,), jnp.float32, 0.0, 1.0)
    return jnp.where(strong, slow_rate, quick_rate)


def draw_token_ids(key, part):
    token_key, reset_key = jax.random.split(key)
    token_draw = jax.random.randint(token_key, (SEQS, LENGTH), 1, VOCAB)
    reset_at = jax.random.randint(reset_key, (SEQS, 1), 1, LENGTH)
    return jnp.where(jnp.arange(LENGTH)[None, :] == reset_at, 0, token_draw).astype(jnp.int32)


def plant(drawn, stream_key, low, largest):
    place = [jax.random.randint(jax.random.fold_in(stream_key, axis), (), 0, length) for axis, length in enumerate(drawn.shape)]
    main_axis = drawn.shape.index(max(drawn.shape))
    beside = place[:main_axis] + [(place[main_axis] + 1) % drawn.shape[main_axis]] + place[main_axis + 1:]
    return drawn.at[tuple(place)].set(low).at[tuple(beside)].set(largest)


def spiked(result, own_key, source, target, parts, factor):
    owner, partner = [(jnp.arange(result.shape[axis_at]) // (result.shape[axis_at] // parts)).reshape([-1 if axis == axis_at else 1 for axis in range(result.ndim)]) for axis_at in (source, target)]
    chosen = jax.random.permutation(own_key, parts)[partner]
    strong = (owner == chosen) | (owner == (partner + parts // 2) % parts)
    return jnp.where(strong, factor * result, result)


def steps_of(own_key, dims, cuts, least, high):
    factor_of, own = 1.0, jax.random.fold_in(own_key, 6)
    for axis_at, blocks in cuts:
        steps = jnp.exp(jax.random.uniform(jax.random.fold_in(own, axis_at), (blocks,), jnp.float32, least / len(cuts), high / len(cuts)))
        factor_of = factor_of * jnp.repeat(steps, dims[axis_at] // blocks).reshape([-1 if axis == axis_at else 1 for axis in range(len(dims))])
    return factor_of


def scatter_about(stream_key, shape, scale, reach, cuts=(), kind=jnp.bfloat16):
    result = jax.random.normal(stream_key, shape, jnp.float32) * scale
    if len(cuts) > 0:
        result = steps_of(stream_key, shape, cuts, -0.22, 0.18) * result
    return jnp.clip(result, min=-reach, max=reach).astype(kind)


def gaussian_with(key, dims, scale, bound, cuts, heavy, dtype=jnp.bfloat16):
    entries = scale * jax.random.normal(key, dims, jnp.float32)
    if cuts:
        entries = entries * steps_of(key, dims, cuts, -0.22, 0.18)
    return jnp.clip(spiked(entries, jax.random.fold_in(key, 3), *heavy), -bound, bound).astype(dtype)


def setup_inputs(seed: int = 0) -> dict:
    arg_keys = jax.random.split(jax.random.key(seed), 13)
    return {
        "head_inputs": scatter_about(arg_keys[0], (SEQS, LENGTH, DI), 1.0, 6.0, ((0, 4), (1, 8))),
        "gate_inputs": gaussian_with(arg_keys[1], (SEQS, LENGTH, DI), 1.0, 6.0, ((0, 4), (1, 8)), (1, 2, 8, 2.0)),
        "state_proj": scatter_about(arg_keys[2], (SEQS, LENGTH, 2 * N), 0.3, 2.0, ((0, 4), (1, 8))),
        "time_steps": draw_time_steps(jax.random.fold_in(arg_keys[12], 71), 0),
        "token_ids": draw_token_ids(jax.random.fold_in(arg_keys[12], 71), 0),
        "token_counts": plant(jax.random.randint(arg_keys[5], (SEQS,), LENGTH // 2, LENGTH + 1), jax.random.fold_in(arg_keys[5], 1), LENGTH // 2, LENGTH).astype(jnp.int32),
        "teacher_out": scatter_about(arg_keys[6], (SEQS, LENGTH, D), 1.0, 6.0, ((0, 4), (1, 8))),
        "out_weight": scatter_about(arg_keys[7], (DI, D), DI ** -0.5, 0.1875, ((0, 32),), jnp.float32),
        "decay_log": draw_decay_log(jax.random.fold_in(arg_keys[12], 71), 0),
        "step_bias": jnp.clip(jax.random.uniform(arg_keys[9], (H,), jnp.float32, -5.0, -3.0), -5.0, -3.0),
        "skip_gain": jnp.clip(jax.random.uniform(arg_keys[10], (H,), jnp.float32, 0.5, 1.5), 0.5, 1.5),
        "norm_gain": jnp.clip(1.0 + 0.1 * jax.random.normal(arg_keys[11], (DI,), jnp.float32), 0.5, 1.5),
    }


norm_floor = 1.0
clip_limit = 1.0
learn_rate = 8.0
highest = lax.Precision.HIGHEST
masked_low = -10000.0

def step_sizes(decay_log, step_bias, step_raw):
    step_width = jax.nn.softplus(step_raw + step_bias[None, :])
    decay_sum = jnp.cumsum(step_width * (-jnp.exp(decay_log))[None, :], axis=0)
    return (step_width, decay_sum)

def mix_block(decay_log, step_bias, skip_gain, norm_gain, state_in, head_inputs, gate_inputs, b_proj, c_proj, step_raw, segment):
    positions = head_inputs.shape[0]
    head_count = decay_log.shape[0]
    step_width, decay_sum = step_sizes(decay_log, step_bias, step_raw)
    inputs_f = head_inputs.astype(jnp.float32).reshape(positions, head_count, -1)
    scaled = inputs_f * step_width[:, :, None]
    scores = jnp.dot(c_proj, b_proj.T, preferred_element_type=jnp.float32)
    position = jnp.arange(positions)
    allowed = (segment[:, None] == segment[None, :]) & (position[:, None] >= position[None, :])

    def one_head(head_data):
        head_sum, head_scaled = head_data
        spread = head_sum[:, None] - head_sum[None, :]
        decay_grid = jnp.exp(jnp.where(allowed, spread, masked_low))
        return jnp.dot(decay_grid * scores, head_scaled, precision=highest)
    intra_sum = jnp.transpose(lax.map(one_head, (decay_sum.T, jnp.transpose(scaled, (1, 0, 2)))), (1, 0, 2))
    entry_decay = jnp.exp(decay_sum) * (segment == 0)[:, None]
    carried = jnp.einsum('in,hpn->ihp', c_proj.astype(jnp.float32), state_in, precision=highest) * entry_decay[:, :, None]
    mixed_out = intra_sum + carried + skip_gain[None, :, None] * inputs_f
    gated = mixed_out.reshape(positions, -1) * jax.nn.silu(gate_inputs.astype(jnp.float32))
    mean_square = lax.optimization_barrier(jnp.mean(gated * gated, axis=1, keepdims=True))
    return gated * norm_gain[None, :] * lax.rsqrt(mean_square + norm_floor)

def state_block(decay_log, step_bias, head_inputs, b_proj, step_raw, segment):
    positions = head_inputs.shape[0]
    head_count = decay_log.shape[0]
    step_width, decay_sum = step_sizes(decay_log, step_bias, step_raw)
    final_sum = decay_sum[-1]
    same_doc = (segment == segment[-1])[:, None]
    tail_decay = jnp.exp(jnp.where(same_doc, final_sum[None, :] - decay_sum, masked_low))
    inputs_f = head_inputs.astype(jnp.float32).reshape(positions, head_count, -1)
    weighted = inputs_f * (step_width * tail_decay)[:, :, None]
    state_out = jnp.einsum('jhp,jn->hpn', weighted, b_proj.astype(jnp.float32), precision=highest)
    carry_out = jnp.exp(final_sum) * (segment[-1] == 0)
    return (carry_out, state_out)

def kahan_total(partials):

    def add_one(running, element):
        summed_up, correction = running
        adjusted = element - correction
        new_total = summed_up + adjusted
        correction = new_total - summed_up - adjusted
        return ((new_total, correction), None)
    (summed_up, correction), _ = lax.scan(add_one, (jnp.zeros((), jnp.float32), jnp.zeros((), jnp.float32)), partials)
    return summed_up

def reference(head_inputs, gate_inputs, state_proj, time_steps, token_ids, token_counts, teacher_out, out_weight, decay_log, step_bias, skip_gain, norm_gain):
    seq_count, length, inner_width = head_inputs.shape
    state_size = state_proj.shape[2] // 2
    model_width = teacher_out.shape[2]
    blocks = N_SEQ
    block_len = length // blocks
    head_count = decay_log.shape[0]
    head_size = inner_width // head_count

    def split_blocks(array):
        return array.reshape((seq_count, blocks, block_len) + array.shape[2:])
    starts = (token_ids == 0).astype(jnp.int32)
    segments = jnp.cumsum(split_blocks(starts), axis=2).astype(jnp.int32)
    position = jnp.arange(length).astype(jnp.int32)
    scored_all = (position[None, :] < token_counts[:, None]).astype(jnp.float32)
    total_count = jnp.sum(token_counts).astype(jnp.float32)
    pieces = (split_blocks(head_inputs), split_blocks(gate_inputs), split_blocks(state_proj), split_blocks(time_steps), segments)
    losses = []
    for step_index in range(STEPS):
        weight_b = out_weight.astype(jnp.bfloat16)
        params = (decay_log, step_bias, skip_gain, norm_gain)

        def one_sequence(running, seq_data):
            sequence, target_s, scored_s = seq_data

            def forward(params_in):

                def per_block(state_in, block_data):
                    inputs_b, gates_b, proj_b, raw_b, seg_b = block_data
                    normed_blk = mix_block(params_in[0], params_in[1], params_in[2], params_in[3], state_in, inputs_b, gates_b, proj_b[:, :state_size], proj_b[:, state_size:], raw_b, seg_b)
                    carry_out, state_out = state_block(params_in[0], params_in[1], inputs_b, proj_b[:, :state_size], raw_b, seg_b)
                    return (carry_out[:, None, None] * state_in + state_out, normed_blk)
                start_state = jnp.zeros((head_count, head_size, state_size), jnp.float32)
                _, normed_seq = lax.scan(jax.checkpoint(per_block), start_state, sequence)
                return normed_seq
            normed, pull_back = jax.vjp(forward, params)
            normed_b = normed.astype(jnp.bfloat16).reshape(-1, inner_width)
            output = jnp.dot(normed_b, weight_b, preferred_element_type=jnp.float32)
            residual = output - target_s.astype(jnp.float32)
            token_loss = lax.optimization_barrier(jnp.sum(residual * residual, axis=1)) * scored_s / model_width
            block_sums = lax.optimization_barrier(jnp.sum(token_loss.reshape(blocks, block_len), axis=1))
            out_grad = (residual * (2.0 / (model_width * total_count)) * scored_s[:, None]).astype(jnp.bfloat16)
            weight_part = jnp.dot(normed_b.T, out_grad, preferred_element_type=jnp.float32)
            normed_grad = jnp.dot(out_grad, weight_b.T, preferred_element_type=jnp.float32).reshape(normed.shape)
            small_part, = pull_back(normed_grad)
            new_running = (running[0] + weight_part, tuple((left + right for left, right in zip(running[1], small_part))))
            return (new_running, block_sums)
        start_running = (jnp.zeros(out_weight.shape, jnp.float32), tuple((jnp.zeros(member.shape, jnp.float32) for member in params)))
        (weight_grad, small_grads), partial_sums = lax.scan(one_sequence, start_running, (pieces, teacher_out, scored_all))
        losses.append(kahan_total(partial_sums.reshape(-1)) / total_count)
        norm_square = jnp.sum(weight_grad * weight_grad) + sum((jnp.sum(member * member) for member in small_grads))
        factor = clip_limit / jnp.maximum(jnp.sqrt(norm_square), clip_limit)
        out_weight = out_weight - learn_rate * factor * weight_grad
        decay_log = decay_log - learn_rate * factor * small_grads[0]
        step_bias = step_bias - learn_rate * factor * small_grads[1]
        skip_gain = skip_gain - learn_rate * factor * small_grads[2]
        norm_gain = norm_gain - learn_rate * factor * small_grads[3]
    return (jnp.stack(losses), out_weight, decay_log, step_bias, skip_gain, norm_gain)
```

```python
import functools

import jax
import jax.numpy as jnp
from jax import lax
from jax.experimental import pallas as pl
from jax.experimental.pallas import tpu as pltpu
from jax.sharding import PartitionSpec as P

STEPS = 2
norm_floor = 1.0
clip_limit = 1.0
learn_rate = 8.0
highest = lax.Precision.HIGHEST
f32 = jnp.float32
bf16 = jnp.bfloat16
LANES = 128
VMEM = pl.BlockSpec(memory_space=pltpu.VMEM)
MESH = pl.DeviceIdType.MESH
LIMIT = 60 * 1024 * 1024


def dot(a, b, **kw):
    return jnp.dot(a, b, preferred_element_type=f32, **kw)


def spread_matrix(heads, width):
    size = width // heads
    lane = lax.broadcasted_iota(jnp.int32, (heads, width), 1)
    head = lax.broadcasted_iota(jnp.int32, (heads, width), 0)
    return ((lane >= head * size) & (lane < (head + 1) * size)).astype(bf16)


def split(a):
    high = a.astype(bf16)
    return high, (a - high.astype(f32)).astype(bf16)


def spread(a, ones):
    high, low = split(a)
    return dot(high, ones) + dot(low, ones)


def head_sum(a, ones):
    high, low = split(a)
    turn = (((1,), (1,)), ((), ()))
    one = functools.partial(
        lax.dot_general, dimension_numbers=turn, preferred_element_type=f32
    )
    return one(high, ones) + one(low, ones)


def column(row):
    n = row.shape[1]
    i = lax.broadcasted_iota(jnp.int32, (n, n), 0)
    j = lax.broadcasted_iota(jnp.int32, (n, n), 1)
    return jnp.sum(jnp.where(i == j, row, 0.0), axis=1, keepdims=True)


def gain_rows(width):
    return width // LANES


def state_kernel(
    pack, raw, raw_t, ids_c, ids_r, x, b_t, sums, sums_t, width, seg_c, seg_r, state, carry
):
    tokens, heads = raw.shape
    inner = x.shape[1]
    g = gain_rows(inner)
    ones = spread_matrix(heads, inner)
    rate_row = -jnp.exp(pack[g : g + 1, :heads])
    bias_row = pack[g + 1 : g + 2, :heads]
    w = jax.nn.softplus(raw[...] + bias_row)
    w_t = jax.nn.softplus(raw_t[...] + column(bias_row))
    i = lax.broadcasted_iota(jnp.int32, (tokens, tokens), 0)
    j = lax.broadcasted_iota(jnp.int32, (tokens, tokens), 1)
    lower = (i >= j).astype(f32)
    upper = (i <= j).astype(f32)
    s = dot(lower, w * rate_row, precision=highest)
    sums[...] = s
    sums_t[...] = dot(w_t * column(rate_row), upper, precision=highest)
    width[...] = w
    sc = jnp.sum(jnp.where((i >= j) & (ids_r[...] == 0), 1.0, 0.0), axis=1, keepdims=True)
    sr = jnp.sum(jnp.where((i <= j) & (ids_c[...] == 0), 1.0, 0.0), axis=0, keepdims=True)
    seg_c[...] = sc
    seg_r[...] = sr
    last = sc[tokens - 1 : tokens, :]
    final = s[tokens - 1 : tokens, :]
    tail = jnp.where(sc == last, jnp.exp(final - s), 0.0)
    weighted = (x[...].astype(f32) * spread(w * tail, ones)).astype(bf16)
    state[...] = dot(b_t[...], weighted).astype(bf16)
    kept = jnp.where(last == 0.0, jnp.exp(final), 0.0)
    carry[...] = spread(jnp.broadcast_to(kept, (8, heads)), ones)[0:1, :]


def mix_kernel(
    pack, sums, sums_t, width, seg_c, seg_r, x, z, b, c, b_t, c_t, target, weight, state,
    scored, scale,
    weight_grad, state_grad, row_dot, col_dot, small, loss,
    scaled, mixed, slope_b, prod,
):
    tokens, heads = sums.shape
    inner = x.shape[1]
    g = gain_rows(inner)
    per = LANES // (inner // heads)
    size = inner // heads
    ones = spread_matrix(heads, inner)
    s = sums[...]
    xf = x[...].astype(f32)
    scaled[...] = (xf * spread(width[...], ones)).astype(bf16)
    i = lax.broadcasted_iota(jnp.int32, (tokens, tokens), 0)
    j = lax.broadcasted_iota(jnp.int32, (tokens, tokens), 1)
    same = seg_c[...] == seg_r[...]
    scores = jnp.where(same & (i >= j), dot(c[...], b_t[...]), 0.0)
    entry = spread(jnp.where(seg_c[...] == 0.0, jnp.exp(s), 0.0), ones)
    mixed[...] = dot(c[...], state[...]) * entry
    lane = lax.broadcasted_iota(jnp.int32, (LANES, LANES), 1)
    for k in range(inner // LANES):
        cols = slice(k * LANES, (k + 1) * LANES)
        for at in range(0, tokens, LANES):
            rows = slice(at, at + LANES)
            end = at + LANES
            total = None
            for p in range(per):
                h = k * per + p
                gap = sums[rows, h : h + 1] - sums_t[h : h + 1, :end]
                grid = (jnp.exp(jnp.minimum(gap, 0.0)) * scores[rows, :end]).astype(bf16)
                part = dot(grid, scaled[:end, cols])
                total = part if total is None else jnp.where(lane < p * size, total, part)
            mixed[rows, cols] += total
    gain = jnp.concatenate([pack[k : k + 1, :] for k in range(g)], axis=1)
    skip = spread(jnp.broadcast_to(pack[g + 2 : g + 3, :heads], (8, heads)), ones)[0:1, :]
    zf = z[...].astype(f32)
    silu = zf * jax.nn.sigmoid(zf)
    gated = (mixed[...] + skip * xf) * silu
    root = lax.rsqrt(jnp.mean(gated * gated, axis=1, keepdims=True) + norm_floor)
    normed = (gated * gain * root).astype(bf16)
    residual = dot(normed, weight[...]) - target[...].astype(f32)
    token_loss = jnp.sum(residual * residual, axis=1, keepdims=True) * scored[...]
    loss[...] = jnp.sum(token_loss, axis=0, keepdims=True) / target.shape[1]
    out_grad = (residual * scale[...]).astype(bf16)
    weight_grad[...] = lax.dot_general(
        normed, out_grad, (((0,), (0,)), ((), ())), preferred_element_type=f32
    ).astype(bf16)
    normed_grad = lax.dot_general(
        out_grad, weight[...], (((1,), (1,)), ((), ())), preferred_element_type=f32
    )
    lifted = normed_grad * gated
    gain_grad = jnp.sum(lifted * root, axis=0, keepdims=True)
    inward = jnp.sum(lifted * gain, axis=1, keepdims=True) * (root * root * root / inner)
    dy = (normed_grad * gain * root - gated * inward) * silu
    small[0:1, :] = gain_grad
    small[1:2, :] = jnp.sum(dy * xf, axis=0, keepdims=True)
    row_dot[...] = head_sum(dy * mixed[...], ones)
    state_grad[...] = dot(c_t[...], (entry * dy).astype(bf16)).astype(bf16)
    slope_b[...] = dy.astype(bf16)
    scores_t = dot(b[...], c_t[...])
    same_t = (seg_c[...] == seg_r[...]) & (i <= j)
    scores_t = jnp.where(same_t, scores_t, 0.0)
    for k in range(inner // LANES):
        cols = slice(k * LANES, (k + 1) * LANES)
        for at in range(0, tokens, LANES):
            rows = slice(at, at + LANES)
            total = None
            for p in range(per):
                h = k * per + p
                gap = sums_t[h : h + 1, at:] - sums[rows, h : h + 1]
                grid = (jnp.exp(jnp.minimum(gap, 0.0)) * scores_t[rows, at:]).astype(bf16)
                part = dot(grid, slope_b[at:, cols])
                total = part if total is None else jnp.where(lane < p * size, total, part)
            prod[rows, cols] = total * x[rows, cols].astype(f32)
    col_dot[...] = head_sum(prod[...], ones)


def back_kernel(
    pack, raw, sums, width, seg_c, x, b, after, state, carry, row_dot, col_dot, small, loss,
    grad_rows, out,
):
    tokens, heads = sums.shape
    inner = x.shape[1]
    g = gain_rows(inner)
    ones = spread_matrix(heads, inner)
    s = sums[...]
    w = width[...]
    rate_row = -jnp.exp(pack[g : g + 1, :heads])
    bias_row = pack[g + 1 : g + 2, :heads]
    sc = seg_c[...]
    last = sc[tokens - 1 : tokens, :]
    final = s[tokens - 1 : tokens, :]
    tail = jnp.where(sc == last, jnp.exp(final - s), 0.0)
    pulled = head_sum(dot(b[...], after[...]) * x[...].astype(f32), ones) * tail
    moved = after[...].astype(f32) * state[...].astype(f32)
    both = jnp.concatenate(
        [
            jnp.sum(moved, axis=0, keepdims=True) * carry[...],
            small[1:2, :],
            jnp.zeros((6, inner), f32),
        ],
        axis=0,
    )
    both = head_sum(both, ones)
    col = col_dot[...] + pulled
    d_sums = row_dot[...] - w * col
    d_final = jnp.sum(w * pulled, axis=0, keepdims=True) + both[0:1, :]
    i = lax.broadcasted_iota(jnp.int32, (tokens, tokens), 0)
    j = lax.broadcasted_iota(jnp.int32, (tokens, tokens), 1)
    d_rate = dot((i <= j).astype(f32), d_sums, precision=highest) + d_final
    d_width = (col + rate_row * d_rate) * jax.nn.sigmoid(raw[...] + bias_row)
    rows = grad_rows[...]
    square = jnp.sum(jnp.sum(rows * rows, axis=1, keepdims=True), axis=0, keepdims=True)
    out[...] = jnp.zeros(out.shape, f32)
    for k in range(g):
        out[k : k + 1, :] = small[0:1, k * LANES : (k + 1) * LANES]
    out[g : g + 1, :heads] = rate_row * jnp.sum(d_rate * w, axis=0, keepdims=True)
    out[g + 1 : g + 2, :heads] = jnp.sum(d_width, axis=0, keepdims=True)
    out[g + 2 : g + 3, :heads] = both[1:2, :]
    out[g + 3 : g + 4, :] = jnp.broadcast_to(loss[...], (1, LANES))
    out[g + 4 : g + 5, :] = jnp.broadcast_to(square, (1, LANES))


def place(flat, n_seq):
    return (flat // n_seq, flat % n_seq)


def meet(n_dp, n_seq):
    n = n_dp * n_seq
    me = lax.axis_index("dp") * n_seq + lax.axis_index("seq")
    barrier = pltpu.get_barrier_semaphore()

    def one(t, _):
        pl.semaphore_signal(
            barrier, inc=1, device_id=place((me + t) % n, n_seq), device_id_type=MESH
        )
        return 0

    lax.fori_loop(1, n, one, 0)
    pl.semaphore_wait(barrier, n - 1)
    return me


def flat_copy(n, n_seq, me, t, source, target, send, recv):
    peer = (me + t) % n
    return pltpu.make_async_remote_copy(
        src_ref=source(peer),
        dst_ref=target.at[me],
        send_sem=send.at[t],
        recv_sem=recv.at[t],
        device_id=place(peer, n_seq),
        device_id_type=MESH,
    )


def flat_arrival(n, n_seq, me, t, source, target, send, recv):
    peer = (me + n - t) % n
    return pltpu.make_async_remote_copy(
        src_ref=source(peer),
        dst_ref=target.at[peer],
        send_sem=send.at[t],
        recv_sem=recv.at[t],
        device_id=place(peer, n_seq),
        device_id_type=MESH,
    )


def seq_copy(n_seq, t, source, target, send, recv):
    mine = lax.axis_index("seq")
    peer = (mine + t) % n_seq
    return pltpu.make_async_remote_copy(
        src_ref=source(peer),
        dst_ref=target.at[mine],
        send_sem=send.at[t],
        recv_sem=recv.at[t],
        device_id=(lax.axis_index("dp"), peer),
        device_id_type=MESH,
    )


def seq_arrival(n_seq, t, source, target, send, recv):
    mine = lax.axis_index("seq")
    peer = (mine + n_seq - t) % n_seq
    return pltpu.make_async_remote_copy(
        src_ref=source(peer),
        dst_ref=target.at[peer],
        send_sem=send.at[t],
        recv_sem=recv.at[t],
        device_id=(lax.axis_index("dp"), peer),
        device_id_type=MESH,
    )


def each(n, body):
    def one(t, _):
        body(t)
        return 0

    lax.fori_loop(1, n, one, 0)


def gather_kernel(
    n_dp, n_seq, rows_b, state, carry, full, entering, carries,
    landed, ready, w_send, w_recv, s_send, s_recv, c_send, c_recv, r_send, r_recv,
):
    n = n_dp * n_seq
    me = meet(n_dp, n_seq)
    mine = lax.axis_index("seq")
    first = (n_seq, lambda p: state.at[p], landed, s_send, s_recv)
    lead = (n_seq, lambda p: carry, carries, c_send, c_recv)
    second = (n_seq, lambda p: ready.at[p], entering, r_send, r_recv)
    whole = (lambda p: rows_b, full, w_send, w_recv)
    go = lambda a, t: (a[0], t) + a[1:]

    def start(t):
        seq_copy(*go(lead, t)).start()
        seq_copy(*go(first, t)).start()

    each(n_seq, start)
    each(n, lambda t: flat_copy(n, n_seq, me, t, *whole).start())
    full[me] = rows_b[...]
    carries[mine] = carry[...]
    landed[mine] = state[mine]

    def arrive(t):
        seq_arrival(*go(lead, t)).wait_recv()
        seq_arrival(*go(first, t)).wait_recv()

    each(n_seq, arrive)
    running = jnp.zeros(state.shape[1:], f32)
    for d in range(n_seq):
        ready[d] = running.astype(bf16)
        if d < n_seq - 1:
            running = carries[d] * running + landed[d].astype(f32)
    each(n_seq, lambda t: seq_copy(*go(second, t)).start())
    entering[mine] = ready[mine]
    each(n_seq, lambda t: seq_arrival(*go(second, t)).wait_recv())
    each(n, lambda t: flat_arrival(n, n_seq, me, t, *whole).wait_recv())

    def sent(t):
        seq_copy(*go(lead, t)).wait_send()
        seq_copy(*go(first, t)).wait_send()
        seq_copy(*go(second, t)).wait_send()

    each(n_seq, sent)
    each(n, lambda t: flat_copy(n, n_seq, me, t, *whole).wait_send())


def scatter_kernel(
    n_dp, n_seq, grad, state, carries, total, leaving,
    parts, landed, ready, w_send, w_recv, s_send, s_recv, r_send, r_recv,
):
    n = n_dp * n_seq
    me = meet(n_dp, n_seq)
    mine = lax.axis_index("seq")
    first = (n_seq, lambda p: state.at[p], landed, s_send, s_recv)
    second = (n_seq, lambda p: ready.at[p], leaving, r_send, r_recv)
    whole = (lambda p: grad.at[p], parts, w_send, w_recv)
    go = lambda a, t: (a[0], t) + a[1:]
    each(n_seq, lambda t: seq_copy(*go(first, t)).start())
    each(n, lambda t: flat_copy(n, n_seq, me, t, *whole).start())
    landed[mine] = state[mine]
    total[...] = grad[me].astype(f32)
    each(n_seq, lambda t: seq_arrival(*go(first, t)).wait_recv())
    running = jnp.zeros(state.shape[1:], f32)
    for d in reversed(range(n_seq)):
        ready[d] = running.astype(bf16)
        if d > 0:
            running = carries[d] * running + landed[d].astype(f32)
    each(n_seq, lambda t: seq_copy(*go(second, t)).start())
    leaving[mine] = ready[mine]

    def add(t):
        flat_arrival(n, n_seq, me, t, *whole).wait_recv()
        total[...] += parts[(me + n - t) % n].astype(f32)

    each(n, add)
    each(n_seq, lambda t: seq_arrival(*go(second, t)).wait_recv())

    def sent(t):
        seq_copy(*go(first, t)).wait_send()
        seq_copy(*go(second, t)).wait_send()

    each(n_seq, sent)
    each(n, lambda t: flat_copy(n, n_seq, me, t, *whole).wait_send())


def update_kernel(
    n_dp, n_seq, inner, part, pack, rows, grad_rows, new_pack, new_rows, rows_b, loss,
    parts, send, recv,
):
    n = n_dp * n_seq
    me = meet(n_dp, n_seq)
    whole = (lambda p: part, parts, send, recv)
    each(n, lambda t: flat_copy(n, n_seq, me, t, *whole).start())
    parts[me] = part[...]
    each(n, lambda t: flat_arrival(n, n_seq, me, t, *whole).wait_recv())
    g = gain_rows(inner)
    summed = lax.fori_loop(1, n, lambda k, acc: acc + parts[k], parts[0])
    at = lax.broadcasted_iota(jnp.int32, summed.shape, 0)
    grads = jnp.where(at < g + 3, summed, 0.0)
    lane_sum = jnp.sum(grads * grads, axis=0, keepdims=True)
    norm_square = jnp.sum(lane_sum, axis=1, keepdims=True) + summed[g + 4 : g + 5, 0:1]
    factor = clip_limit / jnp.maximum(jnp.sqrt(norm_square), clip_limit)
    new_pack[...] = pack[...] - learn_rate * factor * grads
    fresh = rows[...] - learn_rate * factor * grad_rows[...]
    new_rows[...] = fresh
    rows_b[...] = fresh.astype(bf16)
    loss[...] = summed[g + 3 : g + 4, :]
    each(n, lambda t: flat_copy(n, n_seq, me, t, *whole).wait_send())


def call(body, outs, scratch=(), collective=None):
    extra = {}
    if collective is not None:
        extra = {"collective_id": collective, "has_side_effects": True}

    def run(*args):
        return pl.pallas_call(
            body,
            out_shape=tuple(jax.ShapeDtypeStruct(*o) for o in outs),
            in_specs=[VMEM] * len(args),
            out_specs=tuple([VMEM] * len(outs)),
            scratch_shapes=list(scratch),
            compiler_params=pltpu.CompilerParams(vmem_limit_bytes=LIMIT, **extra),
        )(*args)

    return run


def per_device(
    n_dp,
    n_seq,
    head_inputs,
    gate_inputs,
    state_proj,
    time_steps,
    token_ids,
    token_counts,
    teacher_out,
    out_weight,
    decay_log,
    step_bias,
    skip_gain,
    norm_gain,
):
    n = n_dp * n_seq
    x, z, target, raw = head_inputs[0], gate_inputs[0], teacher_out[0], time_steps[0]
    tokens, inner = x.shape
    ns = state_proj.shape[2] // 2
    heads = decay_log.shape[0]
    model = target.shape[1]
    share = out_weight.shape[0]
    piece = ns // n_seq
    g = gain_rows(inner)
    pack_rows = -(-(g + 5) // 8) * 8
    b, c = state_proj[0, :, :ns], state_proj[0, :, ns:]
    both_t = state_proj[0].T
    b_t, c_t = both_t[:ns], both_t[ns:]
    raw_t = raw.T
    ids_r = token_ids
    ids_c = token_ids.reshape(tokens, 1)
    position = lax.axis_index("seq") * tokens + jnp.arange(tokens, dtype=jnp.int32)
    own_count = lax.dynamic_index_in_dim(token_counts, lax.axis_index("dp"), keepdims=False)
    scored = (position < own_count).astype(f32)[:, None]
    total_count = jnp.sum(token_counts).astype(f32)
    scale = scored * (2.0 / (model * total_count))
    wide = lambda a: jnp.pad(a, (0, LANES - heads))[None]
    pack = jnp.concatenate(
        [
            norm_gain.reshape(g, LANES),
            wide(decay_log),
            wide(step_bias),
            wide(skip_gain),
            jnp.zeros((pack_rows - g - 3, LANES), f32),
        ]
    )
    rows = out_weight
    rows_b = rows.astype(bf16)
    dma = pltpu.SemaphoreType.DMA
    losses = []
    per_head = ((tokens, heads), f32)
    for _ in range(STEPS):
        sums, sums_t, width, seg_c, seg_r, state, carry = call(
            state_kernel,
            [
                per_head,
                ((heads, tokens), f32),
                per_head,
                ((tokens, 1), f32),
                ((1, tokens), f32),
                ((ns, inner), bf16),
                ((1, inner), f32),
            ],
        )(pack, raw, raw_t, ids_c, ids_r, x, b_t)
        full, entering, carries = call(
            functools.partial(gather_kernel, n_dp, n_seq),
            [
                ((n, share, model), bf16),
                ((n_seq, piece, inner), bf16),
                ((n_seq, 1, inner), f32),
            ],
            [
                pltpu.VMEM((n_seq, piece, inner), bf16),
                pltpu.VMEM((n_seq, piece, inner), bf16),
                dma((n,)),
                dma((n,)),
            ]
            + [dma((n_seq,))] * 6,
            0,
        )(rows_b, state.reshape(n_seq, piece, inner), carry)
        weight = full.reshape(n * share, model)
        entering = entering.reshape(ns, inner)
        weight_grad, state_grad, row_dot, col_dot, small, loss = call(
            mix_kernel,
            [
                ((inner, model), bf16),
                ((ns, inner), bf16),
                per_head,
                per_head,
                ((8, inner), f32),
                ((1, 1), f32),
            ],
            [
                pltpu.VMEM((tokens, inner), bf16),
                pltpu.VMEM((tokens, inner), f32),
                pltpu.VMEM((tokens, inner), bf16),
                pltpu.VMEM((tokens, inner), f32),
            ],
        )(
            pack, sums, sums_t, width, seg_c, seg_r, x, z, b, c, b_t, c_t, target, weight,
            entering, scored, scale,
        )
        grad_rows, after = call(
            functools.partial(scatter_kernel, n_dp, n_seq),
            [((share, model), f32), ((n_seq, piece, inner), bf16)],
            [
                pltpu.VMEM((n, share, model), bf16),
                pltpu.VMEM((n_seq, piece, inner), bf16),
                pltpu.VMEM((n_seq, piece, inner), bf16),
                dma((n,)),
                dma((n,)),
            ]
            + [dma((n_seq,))] * 4,
            1,
        )(
            weight_grad.reshape(n, share, model),
            state_grad.reshape(n_seq, piece, inner),
            carries,
        )
        part = call(back_kernel, [((pack_rows, LANES), f32)])(
            pack, raw, sums, width, seg_c, x, b, after.reshape(ns, inner), entering, carry,
            row_dot, col_dot, small, loss, grad_rows,
        )[0]
        pack, rows, rows_b, loss_row = call(
            functools.partial(update_kernel, n_dp, n_seq, inner),
            [
                ((pack_rows, LANES), f32),
                ((share, model), f32),
                ((share, model), bf16),
                ((1, LANES), f32),
            ],
            [pltpu.VMEM((n, pack_rows, LANES), f32), dma((n,)), dma((n,))],
            2,
        )(part, pack, rows, grad_rows)
        losses.append(loss_row[0, 0] / total_count)
    return (
        jnp.stack(losses),
        rows,
        pack[g, :heads],
        pack[g + 1, :heads],
        pack[g + 2, :heads],
        pack[:g].reshape(inner),
    )


def solution(mesh):
    in_specs = (
        P("dp", "seq", None),
        P("dp", "seq", None),
        P("dp", "seq", None),
        P("dp", "seq", None),
        P("dp", "seq"),
        P(),
        P("dp", "seq", None),
        P(("dp", "seq"), None),
        P(),
        P(),
        P(),
        P(),
    )
    out_specs = (P(), P(("dp", "seq"), None), P(), P(), P(), P())
    return jax.shard_map(
        functools.partial(per_device, mesh.shape["dp"], mesh.shape["seq"]),
        mesh=mesh,
        in_specs=in_specs,
        out_specs=out_specs,
        check_vma=False,
    )
```

```python
import functools

import jax
import jax.numpy as jnp
from jax import lax
from jax.experimental import pallas as pl
from jax.experimental.pallas import tpu as pltpu
from jax.sharding import PartitionSpec as P

STEPS = 2
norm_floor = 1.0
clip_limit = 1.0
learn_rate = 8.0
highest = lax.Precision.HIGHEST
f32 = jnp.float32
bf16 = jnp.bfloat16
LANES = 128
VMEM = pl.BlockSpec(memory_space=pltpu.VMEM)
SMEM = pl.BlockSpec(memory_space=pltpu.SMEM)
MESH = pl.DeviceIdType.MESH
LIMIT = 60 * 1024 * 1024


def dot(a, b, **kw):
    return jnp.dot(a, b, preferred_element_type=f32, **kw)


def spread_matrix(heads, width):
    size = width // heads
    lane = lax.broadcasted_iota(jnp.int32, (heads, width), 1)
    head = lax.broadcasted_iota(jnp.int32, (heads, width), 0)
    return ((lane >= head * size) & (lane < (head + 1) * size)).astype(bf16)


def split(a):
    high = a.astype(bf16)
    return high, (a - high.astype(f32)).astype(bf16)


def spread(a, ones):
    high, low = split(a)
    return dot(high, ones) + dot(low, ones)


def head_sum(a, ones):
    high, low = split(a)
    turn = (((1,), (1,)), ((), ()))
    one = functools.partial(
        lax.dot_general, dimension_numbers=turn, preferred_element_type=f32
    )
    return one(high, ones) + one(low, ones)


def column(row):
    n = row.shape[1]
    i = lax.broadcasted_iota(jnp.int32, (n, n), 0)
    j = lax.broadcasted_iota(jnp.int32, (n, n), 1)
    return jnp.sum(jnp.where(i == j, row, 0.0), axis=1, keepdims=True)


def gain_rows(width):
    return width // LANES


def state_kernel(
    pack, raw, raw_t, ids_r, x, proj, rows, sums, sums_t, width, seg_c, seg_r, state, carry, rows_b
):
    tokens, heads = raw.shape
    inner = x.shape[1]
    g = gain_rows(inner)
    ones = spread_matrix(heads, inner)
    rate_row = -jnp.exp(pack[g : g + 1, :heads])
    bias_row = pack[g + 1 : g + 2, :heads]
    w = jax.nn.softplus(raw[...] + bias_row)
    w_t = jax.nn.softplus(raw_t[...] + column(bias_row))
    i = lax.broadcasted_iota(jnp.int32, (tokens, tokens), 0)
    j = lax.broadcasted_iota(jnp.int32, (tokens, tokens), 1)
    lower = (i >= j).astype(f32)
    upper = (i <= j).astype(f32)
    s = dot(lower, w * rate_row, precision=highest)
    sums[...] = s
    sums_t[...] = dot(w_t * column(rate_row), upper, precision=highest)
    width[...] = w
    stop = jnp.where(ids_r[...] == 0, 1.0, 0.0)
    sc = jnp.sum(jnp.where(i >= j, stop, 0.0), axis=1, keepdims=True)
    sr = jnp.sum(jnp.where(i <= j, column(stop), 0.0), axis=0, keepdims=True)
    rows_b[...] = rows[...].astype(bf16)
    seg_c[...] = sc
    seg_r[...] = sr
    last = sc[tokens - 1 : tokens, :]
    final = s[tokens - 1 : tokens, :]
    tail = jnp.where(sc == last, jnp.exp(final - s), 0.0)
    weighted = (x[...].astype(f32) * spread(w * tail, ones)).astype(bf16)
    b = proj[:, : proj.shape[1] // 2]
    state[...] = lax.dot_general(
        b, weighted, (((0,), (0,)), ((), ())), preferred_element_type=f32
    ).astype(bf16)
    kept = jnp.where(last == 0.0, jnp.exp(final), 0.0)
    carry[...] = spread(jnp.broadcast_to(kept, (8, heads)), ones)[0:1, :]


def mix_kernel(
    n_dp, counts, pack, sums, sums_t, width, seg_c, seg_r, x, z, proj, target, weight, state,
    weight_grad, state_grad, row_dot, col_dot, small, loss,
    scaled, mixed, slope_b, prod,
):
    tokens, heads = sums.shape
    inner = x.shape[1]
    g = gain_rows(inner)
    per = LANES // (inner // heads)
    size = inner // heads
    ones = spread_matrix(heads, inner)
    s = sums[...]
    xf = x[...].astype(f32)
    scaled[...] = (xf * spread(width[...], ones)).astype(bf16)
    i = lax.broadcasted_iota(jnp.int32, (tokens, tokens), 0)
    j = lax.broadcasted_iota(jnp.int32, (tokens, tokens), 1)
    same = seg_c[...] == seg_r[...]
    ns = proj.shape[1] // 2
    b, c = proj[:, :ns], proj[:, ns:]
    turn = functools.partial(lax.dot_general, preferred_element_type=f32)
    scores = jnp.where(same & (i >= j), turn(c, b, (((1,), (1,)), ((), ()))), 0.0)
    entry = spread(jnp.where(seg_c[...] == 0.0, jnp.exp(s), 0.0), ones)
    mixed[...] = dot(c, state[...]) * entry
    lane = lax.broadcasted_iota(jnp.int32, (LANES, LANES), 1)
    for k in range(inner // LANES):
        cols = slice(k * LANES, (k + 1) * LANES)
        for at in range(0, tokens, LANES):
            rows = slice(at, at + LANES)
            end = at + LANES
            total = None
            for p in range(per):
                h = k * per + p
                gap = sums[rows, h : h + 1] - sums_t[h : h + 1, :end]
                grid = (jnp.exp(jnp.minimum(gap, 0.0)) * scores[rows, :end]).astype(bf16)
                part = dot(grid, scaled[:end, cols])
                total = part if total is None else jnp.where(lane < p * size, total, part)
            mixed[rows, cols] += total
    gain = jnp.concatenate([pack[k : k + 1, :] for k in range(g)], axis=1)
    skip = spread(jnp.broadcast_to(pack[g + 2 : g + 3, :heads], (8, heads)), ones)[0:1, :]
    zf = z[...].astype(f32)
    silu = zf * jax.nn.sigmoid(zf)
    gated = (mixed[...] + skip * xf) * silu
    root = lax.rsqrt(jnp.mean(gated * gated, axis=1, keepdims=True) + norm_floor)
    normed = (gated * gain * root).astype(bf16)
    residual = dot(normed, weight[...]) - target[...].astype(f32)
    model = target.shape[1]
    total_count = counts[0]
    for k in range(1, n_dp):
        total_count = total_count + counts[k]
    share = 1.0 / (model * total_count.astype(f32))
    position = lax.axis_index("seq") * tokens + lax.broadcasted_iota(jnp.int32, (tokens, 1), 0)
    scored = jnp.where(position < counts[lax.axis_index("dp")], 1.0, 0.0)
    token_loss = jnp.sum(residual * residual, axis=1, keepdims=True) * scored
    loss[...] = jnp.sum(token_loss, axis=0, keepdims=True) * share
    out_grad = (residual * (2.0 * share * scored)).astype(bf16)
    weight_grad[...] = lax.dot_general(
        normed, out_grad, (((0,), (0,)), ((), ())), preferred_element_type=f32
    ).astype(bf16)
    normed_grad = lax.dot_general(
        out_grad, weight[...], (((1,), (1,)), ((), ())), preferred_element_type=f32
    )
    lifted = normed_grad * gated
    gain_grad = jnp.sum(lifted * root, axis=0, keepdims=True)
    inward = jnp.sum(lifted * gain, axis=1, keepdims=True) * (root * root * root / inner)
    dy = (normed_grad * gain * root - gated * inward) * silu
    small[0:1, :] = gain_grad
    small[1:2, :] = jnp.sum(dy * xf, axis=0, keepdims=True)
    row_dot[...] = head_sum(dy * mixed[...], ones)
    state_grad[...] = turn(c, (entry * dy).astype(bf16), (((0,), (0,)), ((), ()))).astype(bf16)
    slope_b[...] = dy.astype(bf16)
    scores_t = turn(b, c, (((1,), (1,)), ((), ())))
    same_t = (seg_c[...] == seg_r[...]) & (i <= j)
    scores_t = jnp.where(same_t, scores_t, 0.0)
    for k in range(inner // LANES):
        cols = slice(k * LANES, (k + 1) * LANES)
        for at in range(0, tokens, LANES):
            rows = slice(at, at + LANES)
            total = None
            for p in range(per):
                h = k * per + p
                gap = sums_t[h : h + 1, at:] - sums[rows, h : h + 1]
                grid = (jnp.exp(jnp.minimum(gap, 0.0)) * scores_t[rows, at:]).astype(bf16)
                part = dot(grid, slope_b[at:, cols])
                total = part if total is None else jnp.where(lane < p * size, total, part)
            prod[rows, cols] = total * x[rows, cols].astype(f32)
    col_dot[...] = head_sum(prod[...], ones)


def back_kernel(
    pack, raw, sums, width, seg_c, x, proj, after, state, carry, row_dot, col_dot, small, loss,
    grad_rows, out,
):
    tokens, heads = sums.shape
    inner = x.shape[1]
    g = gain_rows(inner)
    ones = spread_matrix(heads, inner)
    s = sums[...]
    w = width[...]
    rate_row = -jnp.exp(pack[g : g + 1, :heads])
    bias_row = pack[g + 1 : g + 2, :heads]
    sc = seg_c[...]
    last = sc[tokens - 1 : tokens, :]
    final = s[tokens - 1 : tokens, :]
    tail = jnp.where(sc == last, jnp.exp(final - s), 0.0)
    pulled = head_sum(dot(proj[:, : proj.shape[1] // 2], after[...]) * x[...].astype(f32), ones) * tail
    moved = after[...].astype(f32) * state[...].astype(f32)
    both = jnp.concatenate(
        [
            jnp.sum(moved, axis=0, keepdims=True) * carry[...],
            small[1:2, :],
            jnp.zeros((6, inner), f32),
        ],
        axis=0,
    )
    both = head_sum(both, ones)
    col = col_dot[...] + pulled
    d_sums = row_dot[...] - w * col
    d_final = jnp.sum(w * pulled, axis=0, keepdims=True) + both[0:1, :]
    i = lax.broadcasted_iota(jnp.int32, (tokens, tokens), 0)
    j = lax.broadcasted_iota(jnp.int32, (tokens, tokens), 1)
    d_rate = dot((i <= j).astype(f32), d_sums, precision=highest) + d_final
    d_width = (col + rate_row * d_rate) * jax.nn.sigmoid(raw[...] + bias_row)
    rows = grad_rows[...]
    square = jnp.sum(jnp.sum(rows * rows, axis=1, keepdims=True), axis=0, keepdims=True)
    out[...] = jnp.zeros(out.shape, f32)
    for k in range(g):
        out[k : k + 1, :] = small[0:1, k * LANES : (k + 1) * LANES]
    out[g : g + 1, :heads] = rate_row * jnp.sum(d_rate * w, axis=0, keepdims=True)
    out[g + 1 : g + 2, :heads] = jnp.sum(d_width, axis=0, keepdims=True)
    out[g + 2 : g + 3, :heads] = both[1:2, :]
    out[g + 3 : g + 4, :] = jnp.broadcast_to(loss[...], (1, LANES))
    out[g + 4 : g + 5, :] = jnp.broadcast_to(square, (1, LANES))


class Spot:
    def __init__(self, n_dp, n_seq):
        self.n_dp, self.n_seq = n_dp, n_seq
        self.cores = 2 if n_dp % 2 == 0 else 1
        self.ys = n_dp // self.cores
        self.highs = 4 if n_seq % 4 == 0 else n_seq
        self.lows = n_seq // self.highs
        self.dp, self.seq = lax.axis_index("dp"), lax.axis_index("seq")
        self.y, self.core = self.dp // self.cores, self.dp % self.cores
        self.high, self.low = self.seq // self.lows, self.seq % self.lows
        self.me = self.dp * n_seq + self.seq

    def core_peer(self, t):
        return (self.y * self.cores + (self.core + t) % self.cores, self.seq)

    def y_peer(self, t):
        return (((self.y + t) % self.ys) * self.cores + self.core, self.seq)

    def low_peer(self, t):
        return (self.dp, self.high * self.lows + (self.low + t) % self.lows)

    def high_peer(self, t):
        return (self.dp, ((self.high + t) % self.highs) * self.lows + self.low)

    def seq_peer(self, t):
        return (self.dp, (self.seq + t) % self.n_seq)

    def meet(self, with_seq):
        barrier = pltpu.get_barrier_semaphore()
        groups = [(self.cores, self.core_peer), (self.ys, self.y_peer)]
        if with_seq:
            groups.append((self.n_seq, self.seq_peer))
        else:
            groups += [(self.lows, self.low_peer), (self.highs, self.high_peer)]
        for count, peer in groups:
            each(
                count,
                lambda t, peer=peer: pl.semaphore_signal(
                    barrier, inc=1, device_id=peer(t), device_id_type=MESH
                ),
            )
        pl.semaphore_wait(barrier, sum(count - 1 for count, _ in groups))


def each(n, body, first=1):
    def one(t, _):
        body(t)
        return 0

    lax.fori_loop(first, n, one, 0)


def remote(source, target, send, recv, peer):
    return pltpu.make_async_remote_copy(
        src_ref=source,
        dst_ref=target,
        send_sem=send,
        recv_sem=recv,
        device_id=peer,
        device_id_type=MESH,
    )


def gather_kernel(
    n_dp, n_seq, rows_b, state, carry, full, entering, carries,
    landed, ready, own_sem, w_recv, high_send, low_send, y_send, core_send,
    s_send, s_recv, c_send, c_recv, r_send, r_recv,
):
    at = Spot(n_dp, n_seq)
    own = pltpu.make_async_copy(rows_b, full.at[at.me], own_sem)
    own.start()
    at.meet(True)
    mine = at.seq
    back = lambda t: (mine + n_seq - t) % n_seq

    def lead(t):
        return remote(carry, carries.at[mine], c_send.at[t], c_recv.at[t], at.seq_peer(t))

    def lead_in(t):
        return remote(carry, carries.at[back(t)], c_send.at[t], c_recv.at[t], at.seq_peer(t))

    def first(t):
        p = (mine + t) % n_seq
        return remote(state.at[p], landed.at[mine], s_send.at[t], s_recv.at[t], at.seq_peer(t))

    def first_in(t):
        p = back(t)
        return remote(state.at[p], landed.at[p], s_send.at[t], s_recv.at[t], at.seq_peer(t))

    def second(t):
        p = (mine + t) % n_seq
        return remote(ready.at[p], entering.at[mine], r_send.at[t], r_recv.at[t], at.seq_peer(t))

    def second_in(t):
        p = back(t)
        return remote(ready.at[p], entering.at[p], r_send.at[t], r_recv.at[t], at.seq_peer(t))

    def push(chunk, send, peer):
        return remote(full.at[chunk], full.at[chunk], send, w_recv.at[chunk], peer)

    def high_edge(t):
        return push(at.me, high_send.at[t], at.high_peer(t))

    def low_edge(t, high):
        chunk = at.dp * n_seq + high * at.lows + at.low
        return push(chunk, low_send.at[t * at.highs + high], at.low_peer(t))

    def y_edge(t, seq):
        return push(at.dp * n_seq + seq, y_send.at[t * n_seq + seq], at.y_peer(t))

    def core_edge(t, y, seq):
        chunk = (y * at.cores + at.core) * n_seq + seq
        return push(chunk, core_send.at[(t * at.ys + y) * n_seq + seq], at.core_peer(t))

    def arrived(chunk):
        push(chunk, high_send.at[0], at.core_peer(1)).wait_recv()

    def onward(y, seq, to_low, to_y):
        if to_low:
            each(at.lows, lambda t: low_edge(t, seq // at.lows).start())
        if to_y:
            each(at.ys, lambda t: y_edge(t, seq).start())
        each(at.cores, lambda t: core_edge(t, y, seq).start())

    def start(t):
        lead(t).start()
        first(t).start()

    each(n_seq, start)
    own.wait()
    each(at.highs, lambda t: high_edge(t).start())
    onward(at.y, at.seq, True, True)
    carries[mine] = carry[...]
    landed[mine] = state[mine]

    def from_high(t):
        seq = ((at.high + at.highs - t) % at.highs) * at.lows + at.low
        arrived(at.dp * n_seq + seq)
        onward(at.y, seq, True, True)

    each(at.highs, from_high)

    def from_low(t):
        low = (at.low + at.lows - t) % at.lows

        def one(u):
            seq = ((at.high + at.highs - u) % at.highs) * at.lows + low
            arrived(at.dp * n_seq + seq)
            onward(at.y, seq, False, True)

        each(at.highs, one, 0)

    each(at.lows, from_low)

    def arrive(t):
        lead_in(t).wait_recv()
        first_in(t).wait_recv()

    each(n_seq, arrive)
    running = jnp.zeros(state.shape[1:], f32)
    for d in range(n_seq):
        ready[d] = running.astype(bf16)
        if d < n_seq - 1:
            running = carries[d] * running + landed[d].astype(f32)
    each(n_seq, lambda t: second(t).start())
    entering[mine] = ready[mine]

    def from_y(t):
        y = (at.y + at.ys - t) % at.ys

        def one(u):
            high, low = u % at.highs, u // at.highs
            seq = ((at.high + high) % at.highs) * at.lows + (at.low + low) % at.lows
            arrived((y * at.cores + at.core) * n_seq + seq)
            onward(y, seq, False, False)

        each(n_seq, one, 0)

    each(at.ys, from_y)
    each(n_seq, lambda t: second_in(t).wait_recv())

    def from_core(t):
        core = (at.core + t) % at.cores

        def one(k):
            arrived(((k // n_seq) * at.cores + core) * n_seq + k % n_seq)

        each(at.ys * n_seq, one, 0)

    each(at.cores, from_core)

    def sent(t):
        lead(t).wait_send()
        first(t).wait_send()
        second(t).wait_send()

    each(n_seq, sent)
    each(at.highs, lambda t: high_edge(t).wait_send())
    each(at.lows, lambda t: each(at.highs, lambda k: low_edge(t, k).wait_send(), 0))
    each(at.ys, lambda t: each(n_seq, lambda k: y_edge(t, k).wait_send(), 0))
    each(
        at.cores,
        lambda t: each(
            at.ys * n_seq, lambda k: core_edge(t, k // n_seq, k % n_seq).wait_send(), 0
        ),
    )


def scatter_kernel(
    n_dp, n_seq, grad, state, carries, total, leaving,
    staged, from_core, from_y, from_low, from_high, landed, ready,
    core_send, core_recv, y_send, y_recv, low_send, low_recv, high_send, high_recv,
    s_send, s_recv, r_send, r_recv,
):
    at = Spot(n_dp, n_seq)
    at.meet(True)
    mine = at.seq
    back = lambda t: (mine + n_seq - t) % n_seq

    def first(t):
        p = (mine + t) % n_seq
        return remote(state.at[p], landed.at[mine], s_send.at[t], s_recv.at[t], at.seq_peer(t))

    def first_in(t):
        p = back(t)
        return remote(state.at[p], landed.at[p], s_send.at[t], s_recv.at[t], at.seq_peer(t))

    def second(t):
        p = (mine + t) % n_seq
        return remote(ready.at[p], leaving.at[mine], r_send.at[t], r_recv.at[t], at.seq_peer(t))

    def second_in(t):
        p = back(t)
        return remote(ready.at[p], leaving.at[p], r_send.at[t], r_recv.at[t], at.seq_peer(t))

    def core_edge(t, y, seq):
        core = (at.core + t) % at.cores
        k = (t * at.ys + y) * n_seq + seq
        return remote(
            grad.at[(y * at.cores + core) * n_seq + seq], from_core.at[k],
            core_send.at[k], core_recv.at[k], at.core_peer(t),
        )

    def y_edge(t, seq):
        k = t * n_seq + seq
        y = (at.y + t) % at.ys
        return remote(
            staged.at[y * n_seq + seq], from_y.at[k], y_send.at[k], y_recv.at[k], at.y_peer(t)
        )

    def low_edge(t, high):
        k = t * at.highs + high
        seq = high * at.lows + (at.low + t) % at.lows
        return remote(
            staged.at[at.y * n_seq + seq], from_low.at[k],
            low_send.at[k], low_recv.at[k], at.low_peer(t),
        )

    def high_edge(t):
        seq = ((at.high + t) % at.highs) * at.lows + at.low
        return remote(
            staged.at[at.y * n_seq + seq], from_high.at[t],
            high_send.at[t], high_recv.at[t], at.high_peer(t),
        )

    def chip_sum(y, seq):
        acc = grad[(y * at.cores + at.core) * n_seq + seq].astype(f32)
        for t in range(1, at.cores):
            core_edge(t, y, seq).wait_recv()
            acc = acc + from_core[(t * at.ys + y) * n_seq + seq].astype(f32)
        return acc

    def y_sum(seq):
        acc = chip_sum(at.y, seq)
        for t in range(1, at.ys):
            y_edge(t, seq).wait_recv()
            acc = acc + from_y[t * n_seq + seq].astype(f32)
        return acc

    def low_sum(high):
        acc = y_sum(high * at.lows + at.low)
        for t in range(1, at.lows):
            low_edge(t, high).wait_recv()
            acc = acc + from_low[t * at.highs + high].astype(f32)
        return acc

    def order(u):
        low = (at.low + 1 + u // at.highs) % at.lows
        return ((at.high + 1 + u) % at.highs) * at.lows + low

    each(n_seq, lambda t: first(t).start())

    def to_core(t):
        def one(k):
            core_edge(t, (at.y + 1 + k // n_seq) % at.ys, order(k % n_seq)).start()

        each(at.ys * n_seq, one, 0)

    each(at.cores, to_core)
    landed[mine] = state[mine]

    def to_y(t):
        y = (at.y + t) % at.ys

        def one(u):
            seq = order(u)
            staged[y * n_seq + seq] = chip_sum(y, seq).astype(bf16)
            y_edge(t, seq).start()

        each(n_seq, one, 0)

    each(at.ys, to_y)
    each(n_seq, lambda t: first_in(t).wait_recv())
    running = jnp.zeros(state.shape[1:], f32)
    for d in reversed(range(n_seq)):
        ready[d] = running.astype(bf16)
        if d > 0:
            running = carries[d] * running + landed[d].astype(f32)
    each(n_seq, lambda t: second(t).start())
    leaving[mine] = ready[mine]

    def to_low(t):
        def one(u):
            high = (at.high + 1 + u) % at.highs
            seq = high * at.lows + (at.low + t) % at.lows
            staged[at.y * n_seq + seq] = y_sum(seq).astype(bf16)
            low_edge(t, high).start()

        each(at.highs, one, 0)

    each(at.lows, to_low)

    def to_high(t):
        high = (at.high + t) % at.highs
        staged[at.y * n_seq + high * at.lows + at.low] = low_sum(high).astype(bf16)
        high_edge(t).start()

    each(at.highs, to_high)
    acc = low_sum(at.high)
    for t in range(1, at.highs):
        high_edge(t).wait_recv()
        acc = acc + from_high[t].astype(f32)
    total[...] = acc
    each(n_seq, lambda t: second_in(t).wait_recv())

    def sent(t):
        first(t).wait_send()
        second(t).wait_send()

    each(n_seq, sent)
    each(at.highs, lambda t: high_edge(t).wait_send())
    each(at.lows, lambda t: each(at.highs, lambda k: low_edge(t, k).wait_send(), 0))
    each(at.ys, lambda t: each(n_seq, lambda k: y_edge(t, k).wait_send(), 0))
    each(
        at.cores,
        lambda t: each(
            at.ys * n_seq, lambda k: core_edge(t, k // n_seq, k % n_seq).wait_send(), 0
        ),
    )


def update_kernel(
    n_dp, n_seq, inner, part, pack, rows, grad_rows, new_pack, new_rows, loss,
    by_core, by_y, by_low, by_high, send, recv,
):
    at = Spot(n_dp, n_seq)
    at.meet(False)
    summed = part[...]
    levels = [
        (by_core, at.cores, at.core, at.core_peer),
        (by_y, at.ys, at.y, at.y_peer),
        (by_low, at.lows, at.low, at.low_peer),
        (by_high, at.highs, at.high, at.high_peer),
    ]
    base = 0
    for held, count, digit, peer in levels:
        held[digit] = summed

        def edge(t, slot, held=held, digit=digit, peer=peer, base=base):
            return remote(held.at[digit], held.at[slot], send.at[base + t], recv.at[base + t], peer(t))

        each(count, lambda t: edge(t, digit).start())
        each(count, lambda t: edge(t, (digit + count - t) % count).wait_recv())
        summed = held[0]
        for k in range(1, count):
            summed = summed + held[k]
        each(count, lambda t: edge(t, digit).wait_send())
        base += count
    g = gain_rows(inner)
    row = lax.broadcasted_iota(jnp.int32, summed.shape, 0)
    grads = jnp.where(row < g + 3, summed, 0.0)
    lane_sum = jnp.sum(grads * grads, axis=0, keepdims=True)
    norm_square = jnp.sum(lane_sum, axis=1, keepdims=True) + summed[g + 4 : g + 5, 0:1]
    factor = clip_limit / jnp.maximum(jnp.sqrt(norm_square), clip_limit)
    new_pack[...] = pack[...] - learn_rate * factor * grads
    new_rows[...] = rows[...] - learn_rate * factor * grad_rows[...]
    loss[...] = summed[g + 3 : g + 4, :]


def call(body, outs, scratch=(), collective=None):
    extra = {}
    if collective is not None:
        extra = {"collective_id": collective, "has_side_effects": True}

    def run(*args):
        return pl.pallas_call(
            body,
            out_shape=tuple(jax.ShapeDtypeStruct(*o) for o in outs),
            in_specs=[SMEM if a.ndim == 1 else VMEM for a in args],
            out_specs=tuple([VMEM] * len(outs)),
            scratch_shapes=list(scratch),
            compiler_params=pltpu.CompilerParams(vmem_limit_bytes=LIMIT, **extra),
        )(*args)

    return run


def per_device(
    n_dp,
    n_seq,
    head_inputs,
    gate_inputs,
    state_proj,
    time_steps,
    token_ids,
    token_counts,
    teacher_out,
    out_weight,
    decay_log,
    step_bias,
    skip_gain,
    norm_gain,
):
    n = n_dp * n_seq
    x, z, target, raw = head_inputs[0], gate_inputs[0], teacher_out[0], time_steps[0]
    tokens, inner = x.shape
    ns = state_proj.shape[2] // 2
    heads = decay_log.shape[0]
    model = target.shape[1]
    share = out_weight.shape[0]
    piece = ns // n_seq
    g = gain_rows(inner)
    pack_rows = -(-(g + 5) // 8) * 8
    proj = state_proj[0]
    raw_t = raw.T
    ids_r = token_ids
    wide = lambda a: jnp.pad(a, (0, LANES - heads))[None]
    pack = jnp.concatenate(
        [
            norm_gain.reshape(g, LANES),
            wide(decay_log),
            wide(step_bias),
            wide(skip_gain),
            jnp.zeros((pack_rows - g - 3, LANES), f32),
        ]
    )
    rows = out_weight
    dma = pltpu.SemaphoreType.DMA
    losses = []
    per_head = ((tokens, heads), f32)
    for _ in range(STEPS):
        sums, sums_t, width, seg_c, seg_r, state, carry, rows_b = call(
            state_kernel,
            [
                per_head,
                ((heads, tokens), f32),
                per_head,
                ((tokens, 1), f32),
                ((1, tokens), f32),
                ((ns, inner), bf16),
                ((1, inner), f32),
                ((share, model), bf16),
            ],
        )(pack, raw, raw_t, ids_r, x, proj, rows)
        full, entering, carries = call(
            functools.partial(gather_kernel, n_dp, n_seq),
            [
                ((n, share, model), bf16),
                ((n_seq, piece, inner), bf16),
                ((n_seq, 1, inner), f32),
            ],
            [
                pltpu.VMEM((n_seq, piece, inner), bf16),
                pltpu.VMEM((n_seq, piece, inner), bf16),
                dma,
                dma((n,)),
                dma((n_seq,)),
                dma((n_seq * n_seq,)),
                dma((n,)),
                dma((n,)),
            ]
            + [dma((n_seq,))] * 6,
            0,
        )(rows_b, state.reshape(n_seq, piece, inner), carry)
        weight = full.reshape(n * share, model)
        entering = entering.reshape(ns, inner)
        weight_grad, state_grad, row_dot, col_dot, small, loss = call(
            functools.partial(mix_kernel, n_dp),
            [
                ((inner, model), bf16),
                ((ns, inner), bf16),
                per_head,
                per_head,
                ((8, inner), f32),
                ((1, 1), f32),
            ],
            [
                pltpu.VMEM((tokens, inner), bf16),
                pltpu.VMEM((tokens, inner), f32),
                pltpu.VMEM((tokens, inner), bf16),
                pltpu.VMEM((tokens, inner), f32),
            ],
        )(
            token_counts, pack, sums, sums_t, width, seg_c, seg_r, x, z, proj, target, weight,
            entering,
        )
        grad_rows, after = call(
            functools.partial(scatter_kernel, n_dp, n_seq),
            [((share, model), f32), ((n_seq, piece, inner), bf16)],
            [
                pltpu.VMEM((n, share, model), bf16),
                pltpu.VMEM((n, share, model), bf16),
                pltpu.VMEM((n, share, model), bf16),
                pltpu.VMEM((n_seq, share, model), bf16),
                pltpu.VMEM((n_seq, share, model), bf16),
                pltpu.VMEM((n_seq, piece, inner), bf16),
                pltpu.VMEM((n_seq, piece, inner), bf16),
            ]
            + [dma((n,))] * 4
            + [dma((n_seq,))] * 8,
            1,
        )(
            weight_grad.reshape(n, share, model),
            state_grad.reshape(n_seq, piece, inner),
            carries,
        )
        part = call(back_kernel, [((pack_rows, LANES), f32)])(
            pack, raw, sums, width, seg_c, x, proj, after.reshape(ns, inner), entering, carry,
            row_dot, col_dot, small, loss, grad_rows,
        )[0]
        pack, rows, loss_row = call(
            functools.partial(update_kernel, n_dp, n_seq, inner),
            [
                ((pack_rows, LANES), f32),
                ((share, model), f32),
                ((1, LANES), f32),
            ],
            [pltpu.VMEM((k, pack_rows, LANES), f32) for k in (n_dp, n_dp, n_seq, n_seq)]
            + [dma((n,))] * 2,
            2,
        )(part, pack, rows, grad_rows)
        losses.append(loss_row[0, 0])
    return (
        jnp.stack(losses),
        rows,
        pack[g, :heads],
        pack[g + 1, :heads],
        pack[g + 2, :heads],
        pack[:g].reshape(inner),
    )


def solution(mesh):
    in_specs = (
        P("dp", "seq", None),
        P("dp", "seq", None),
        P("dp", "seq", None),
        P("dp", "seq", None),
        P("dp", "seq"),
        P(),
        P("dp", "seq", None),
        P(("dp", "seq"), None),
        P(),
        P(),
        P(),
        P(),
    )
    out_specs = (P(), P(("dp", "seq"), None), P(), P(), P(), P())
    return jax.shard_map(
        functools.partial(per_device, mesh.shape["dp"], mesh.shape["seq"]),
        mesh=mesh,
        in_specs=in_specs,
        out_specs=out_specs,
        check_vma=False,
    )
```

```python
import functools

import jax
import jax.numpy as jnp
from jax import lax
from jax.experimental import pallas as pl
from jax.experimental.pallas import tpu as pltpu
from jax.sharding import PartitionSpec as P

STEPS = 2
norm_floor = 1.0
clip_limit = 1.0
learn_rate = 8.0
highest = lax.Precision.HIGHEST
f32 = jnp.float32
bf16 = jnp.bfloat16
LANES = 128
VMEM = pl.BlockSpec(memory_space=pltpu.VMEM)
SMEM = pl.BlockSpec(memory_space=pltpu.SMEM)
MESH = pl.DeviceIdType.MESH
LIMIT = 60 * 1024 * 1024


def dot(a, b, **kw):
    return jnp.dot(a, b, preferred_element_type=f32, **kw)


def spread_matrix(heads, width):
    size = width // heads
    lane = lax.broadcasted_iota(jnp.int32, (heads, width), 1)
    head = lax.broadcasted_iota(jnp.int32, (heads, width), 0)
    return ((lane >= head * size) & (lane < (head + 1) * size)).astype(bf16)


def split(a):
    high = a.astype(bf16)
    return high, (a - high.astype(f32)).astype(bf16)


def spread(a, ones):
    high, low = split(a)
    return dot(high, ones) + dot(low, ones)


def head_sum(a, ones):
    high, low = split(a)
    turn = (((1,), (1,)), ((), ()))
    one = functools.partial(
        lax.dot_general, dimension_numbers=turn, preferred_element_type=f32
    )
    return one(high, ones) + one(low, ones)


def column(row):
    n = row.shape[1]
    i = lax.broadcasted_iota(jnp.int32, (n, n), 0)
    j = lax.broadcasted_iota(jnp.int32, (n, n), 1)
    return jnp.sum(jnp.where(i == j, row, 0.0), axis=1, keepdims=True)


def gain_rows(width):
    return width // LANES


def state_part(
    pack, raw, raw_t, ids_r, x, proj, sums, sums_t, width, seg_c, seg_r, state, carry
):
    tokens, heads = raw.shape
    inner = x.shape[1]
    g = gain_rows(inner)
    ones = spread_matrix(heads, inner)
    rate_row = -jnp.exp(pack[g : g + 1, :heads])
    bias_row = pack[g + 1 : g + 2, :heads]
    w = jax.nn.softplus(raw[...] + bias_row)
    w_t = jax.nn.softplus(raw_t[...] + column(bias_row))
    i = lax.broadcasted_iota(jnp.int32, (tokens, tokens), 0)
    j = lax.broadcasted_iota(jnp.int32, (tokens, tokens), 1)
    lower = (i >= j).astype(f32)
    upper = (i <= j).astype(f32)
    s = dot(lower, w * rate_row, precision=highest)
    sums[...] = s
    sums_t[...] = dot(w_t * column(rate_row), upper, precision=highest)
    width[...] = w
    stop = jnp.where(ids_r[...] == 0, 1.0, 0.0)
    sc = jnp.sum(jnp.where(i >= j, stop, 0.0), axis=1, keepdims=True)
    sr = jnp.sum(jnp.where(i <= j, column(stop), 0.0), axis=0, keepdims=True)
    seg_c[...] = sc
    seg_r[...] = sr
    last = sc[tokens - 1 : tokens, :]
    final = s[tokens - 1 : tokens, :]
    tail = jnp.where(sc == last, jnp.exp(final - s), 0.0)
    weighted = (x[...].astype(f32) * spread(w * tail, ones)).astype(bf16)
    b = proj[:, : proj.shape[1] // 2]
    ended = lax.dot_general(
        b, weighted, (((0,), (0,)), ((), ())), preferred_element_type=f32
    )
    piece = state.shape[1]
    for p in range(state.shape[0]):
        state[p] = ended[p * piece : (p + 1) * piece].astype(bf16)
    kept = jnp.where(last == 0.0, jnp.exp(final), 0.0)
    carry[...] = spread(jnp.broadcast_to(kept, (8, heads)), ones)[0:1, :]


def mix_kernel(
    n_dp, counts, pack, sums, sums_t, width, seg_c, seg_r, x, z, proj, target, weight, state,
    weight_grad, state_grad, row_dot, col_dot, small, loss,
    scaled, mixed, slope_b, prod,
):
    tokens, heads = sums.shape
    inner = x.shape[1]
    g = gain_rows(inner)
    per = LANES // (inner // heads)
    size = inner // heads
    ones = spread_matrix(heads, inner)
    s = sums[...]
    xf = x[...].astype(f32)
    scaled[...] = (xf * spread(width[...], ones)).astype(bf16)
    i = lax.broadcasted_iota(jnp.int32, (tokens, tokens), 0)
    j = lax.broadcasted_iota(jnp.int32, (tokens, tokens), 1)
    same = seg_c[...] == seg_r[...]
    ns = proj.shape[1] // 2
    b, c = proj[:, :ns], proj[:, ns:]
    turn = functools.partial(lax.dot_general, preferred_element_type=f32)
    scores = jnp.where(same & (i >= j), turn(c, b, (((1,), (1,)), ((), ()))), 0.0)
    entry = spread(jnp.where(seg_c[...] == 0.0, jnp.exp(s), 0.0), ones)
    mixed[...] = dot(c, state[...]) * entry
    lane = lax.broadcasted_iota(jnp.int32, (LANES, LANES), 1)
    for k in range(inner // LANES):
        cols = slice(k * LANES, (k + 1) * LANES)
        for at in range(0, tokens, LANES):
            rows = slice(at, at + LANES)
            end = at + LANES
            total = None
            for p in range(per):
                h = k * per + p
                gap = sums[rows, h : h + 1] - sums_t[h : h + 1, :end]
                grid = (jnp.exp(jnp.minimum(gap, 0.0)) * scores[rows, :end]).astype(bf16)
                part = dot(grid, scaled[:end, cols])
                total = part if total is None else jnp.where(lane < p * size, total, part)
            mixed[rows, cols] += total
    gain = jnp.concatenate([pack[k : k + 1, :] for k in range(g)], axis=1)
    skip = spread(jnp.broadcast_to(pack[g + 2 : g + 3, :heads], (8, heads)), ones)[0:1, :]
    zf = z[...].astype(f32)
    silu = zf * jax.nn.sigmoid(zf)
    gated = (mixed[...] + skip * xf) * silu
    root = lax.rsqrt(jnp.mean(gated * gated, axis=1, keepdims=True) + norm_floor)
    normed = (gated * gain * root).astype(bf16)
    residual = dot(normed, weight[...]) - target[...].astype(f32)
    model = target.shape[1]
    total_count = counts[0]
    for k in range(1, n_dp):
        total_count = total_count + counts[k]
    share = 1.0 / (model * total_count.astype(f32))
    position = lax.axis_index("seq") * tokens + lax.broadcasted_iota(jnp.int32, (tokens, 1), 0)
    scored = jnp.where(position < counts[lax.axis_index("dp")], 1.0, 0.0)
    token_loss = jnp.sum(residual * residual, axis=1, keepdims=True) * scored
    loss[...] = jnp.sum(token_loss, axis=0, keepdims=True) * share
    out_grad = (residual * (2.0 * share * scored)).astype(bf16)
    weight_grad[...] = lax.dot_general(
        normed, out_grad, (((0,), (0,)), ((), ())), preferred_element_type=f32
    ).astype(bf16)
    normed_grad = lax.dot_general(
        out_grad, weight[...], (((1,), (1,)), ((), ())), preferred_element_type=f32
    )
    lifted = normed_grad * gated
    gain_grad = jnp.sum(lifted * root, axis=0, keepdims=True)
    inward = jnp.sum(lifted * gain, axis=1, keepdims=True) * (root * root * root / inner)
    dy = (normed_grad * gain * root - gated * inward) * silu
    small[0:1, :] = gain_grad
    small[1:2, :] = jnp.sum(dy * xf, axis=0, keepdims=True)
    row_dot[...] = head_sum(dy * mixed[...], ones)
    state_grad[...] = turn(c, (entry * dy).astype(bf16), (((0,), (0,)), ((), ()))).astype(bf16)
    slope_b[...] = dy.astype(bf16)
    scores_t = turn(b, c, (((1,), (1,)), ((), ())))
    same_t = (seg_c[...] == seg_r[...]) & (i <= j)
    scores_t = jnp.where(same_t, scores_t, 0.0)
    for k in range(inner // LANES):
        cols = slice(k * LANES, (k + 1) * LANES)
        for at in range(0, tokens, LANES):
            rows = slice(at, at + LANES)
            total = None
            for p in range(per):
                h = k * per + p
                gap = sums_t[h : h + 1, at:] - sums[rows, h : h + 1]
                grid = (jnp.exp(jnp.minimum(gap, 0.0)) * scores_t[rows, at:]).astype(bf16)
                part = dot(grid, slope_b[at:, cols])
                total = part if total is None else jnp.where(lane < p * size, total, part)
            prod[rows, cols] = total * x[rows, cols].astype(f32)
    col_dot[...] = head_sum(prod[...], ones)


def back_part(
    pack, raw, sums, width, seg_c, x, proj, after, state, carry, row_dot, col_dot, small, loss,
    out,
):
    tokens, heads = sums.shape
    inner = x.shape[1]
    g = gain_rows(inner)
    ones = spread_matrix(heads, inner)
    s = sums[...]
    w = width[...]
    rate_row = -jnp.exp(pack[g : g + 1, :heads])
    bias_row = pack[g + 1 : g + 2, :heads]
    sc = seg_c[...]
    last = sc[tokens - 1 : tokens, :]
    final = s[tokens - 1 : tokens, :]
    tail = jnp.where(sc == last, jnp.exp(final - s), 0.0)
    after = jnp.concatenate([after[p].astype(f32) for p in range(after.shape[0])], axis=0)
    pulled = head_sum(dot(proj[:, : proj.shape[1] // 2], after.astype(bf16)) * x[...].astype(f32), ones) * tail
    moved = after * state[...].astype(f32)
    both = jnp.concatenate(
        [
            jnp.sum(moved, axis=0, keepdims=True) * carry[...],
            small[1:2, :],
            jnp.zeros((6, inner), f32),
        ],
        axis=0,
    )
    both = head_sum(both, ones)
    col = col_dot[...] + pulled
    d_sums = row_dot[...] - w * col
    d_final = jnp.sum(w * pulled, axis=0, keepdims=True) + both[0:1, :]
    i = lax.broadcasted_iota(jnp.int32, (tokens, tokens), 0)
    j = lax.broadcasted_iota(jnp.int32, (tokens, tokens), 1)
    d_rate = dot((i <= j).astype(f32), d_sums, precision=highest) + d_final
    d_width = (col + rate_row * d_rate) * jax.nn.sigmoid(raw[...] + bias_row)
    out[...] = jnp.zeros(out.shape, f32)
    for k in range(g):
        out[k : k + 1, :] = small[0:1, k * LANES : (k + 1) * LANES]
    out[g : g + 1, :heads] = rate_row * jnp.sum(d_rate * w, axis=0, keepdims=True)
    out[g + 1 : g + 2, :heads] = jnp.sum(d_width, axis=0, keepdims=True)
    out[g + 2 : g + 3, :heads] = both[1:2, :]
    out[g + 3 : g + 4, :] = jnp.broadcast_to(loss[...], (1, LANES))


class Spot:
    def __init__(self, n_dp, n_seq):
        self.n_dp, self.n_seq = n_dp, n_seq
        self.cores = 2 if n_dp % 2 == 0 else 1
        self.ys = n_dp // self.cores
        self.highs = 4 if n_seq % 4 == 0 else n_seq
        self.lows = n_seq // self.highs
        self.dp, self.seq = lax.axis_index("dp"), lax.axis_index("seq")
        self.y, self.core = self.dp // self.cores, self.dp % self.cores
        self.high, self.low = self.seq // self.lows, self.seq % self.lows
        self.me = self.dp * n_seq + self.seq

    def core_peer(self, t):
        return (self.y * self.cores + (self.core + t) % self.cores, self.seq)

    def y_peer(self, t):
        return (((self.y + t) % self.ys) * self.cores + self.core, self.seq)

    def low_peer(self, t):
        return (self.dp, self.high * self.lows + (self.low + t) % self.lows)

    def high_peer(self, t):
        return (self.dp, ((self.high + t) % self.highs) * self.lows + self.low)

    def seq_peer(self, t):
        return (self.dp, (self.seq + t) % self.n_seq)

    def meet(self, with_seq):
        barrier = pltpu.get_barrier_semaphore()
        groups = [(self.cores, self.core_peer), (self.ys, self.y_peer)]
        if with_seq:
            groups.append((self.n_seq, self.seq_peer))
        else:
            groups += [(self.lows, self.low_peer), (self.highs, self.high_peer)]
        for count, peer in groups:
            each(
                count,
                lambda t, peer=peer: pl.semaphore_signal(
                    barrier, inc=1, device_id=peer(t), device_id_type=MESH
                ),
            )
        pl.semaphore_wait(barrier, sum(count - 1 for count, _ in groups))


def each(n, body, first=1):
    def one(t, _):
        body(t)
        return 0

    lax.fori_loop(first, n, one, 0)


def remote(source, target, send, recv, peer):
    return pltpu.make_async_remote_copy(
        src_ref=source,
        dst_ref=target,
        send_sem=send,
        recv_sem=recv,
        device_id=peer,
        device_id_type=MESH,
    )


def gather_kernel(
    n_dp, n_seq, pack, raw, raw_t, ids_r, x, proj, rows,
    sums, sums_t, width, seg_c, seg_r, carry, full, entering, carries,
    state, landed, ready, w_recv, high_send, low_send, y_send, core_send,
    s_send, s_recv, c_send, c_recv, r_send, r_recv,
):
    at = Spot(n_dp, n_seq)
    full[at.me] = rows[...].astype(bf16)
    at.meet(True)
    mine = at.seq
    back = lambda t: (mine + n_seq - t) % n_seq

    def lead(t):
        return remote(carry, carries.at[mine], c_send.at[t], c_recv.at[t], at.seq_peer(t))

    def lead_in(t):
        return remote(carry, carries.at[back(t)], c_send.at[t], c_recv.at[t], at.seq_peer(t))

    def first(t):
        p = (mine + t) % n_seq
        return remote(state.at[p], landed.at[mine], s_send.at[t], s_recv.at[t], at.seq_peer(t))

    def first_in(t):
        p = back(t)
        return remote(state.at[p], landed.at[p], s_send.at[t], s_recv.at[t], at.seq_peer(t))

    def second(t):
        p = (mine + t) % n_seq
        return remote(ready.at[p], entering.at[mine], r_send.at[t], r_recv.at[t], at.seq_peer(t))

    def second_in(t):
        p = back(t)
        return remote(ready.at[p], entering.at[p], r_send.at[t], r_recv.at[t], at.seq_peer(t))

    def push(chunk, send, peer):
        return remote(full.at[chunk], full.at[chunk], send, w_recv.at[chunk], peer)

    def high_edge(t):
        return push(at.me, high_send.at[t], at.high_peer(t))

    def low_edge(t, high):
        chunk = at.dp * n_seq + high * at.lows + at.low
        return push(chunk, low_send.at[t * at.highs + high], at.low_peer(t))

    def y_edge(t, seq):
        return push(at.dp * n_seq + seq, y_send.at[t * n_seq + seq], at.y_peer(t))

    def core_edge(t, y, seq):
        chunk = (y * at.cores + at.core) * n_seq + seq
        return push(chunk, core_send.at[(t * at.ys + y) * n_seq + seq], at.core_peer(t))

    def arrived(chunk):
        push(chunk, high_send.at[0], at.core_peer(1)).wait_recv()

    def onward(y, seq, to_low, to_y):
        if to_low:
            each(at.lows, lambda t: low_edge(t, seq // at.lows).start())
        if to_y:
            each(at.ys, lambda t: y_edge(t, seq).start())
        each(at.cores, lambda t: core_edge(t, y, seq).start())

    def start(t):
        lead(t).start()
        first(t).start()

    each(at.highs, lambda t: high_edge(t).start())
    onward(at.y, at.seq, True, True)
    state_part(
        pack, raw, raw_t, ids_r, x, proj, sums, sums_t, width, seg_c, seg_r, state, carry
    )
    each(n_seq, start)
    carries[mine] = carry[...]
    landed[mine] = state[mine]

    def from_high(t):
        seq = ((at.high + at.highs - t) % at.highs) * at.lows + at.low
        arrived(at.dp * n_seq + seq)
        onward(at.y, seq, True, True)

    each(at.highs, from_high)

    def from_low(t):
        low = (at.low + at.lows - t) % at.lows

        def one(u):
            seq = ((at.high + at.highs - u) % at.highs) * at.lows + low
            arrived(at.dp * n_seq + seq)
            onward(at.y, seq, False, True)

        each(at.highs, one, 0)

    each(at.lows, from_low)

    def arrive(t):
        lead_in(t).wait_recv()
        first_in(t).wait_recv()

    each(n_seq, arrive)
    running = jnp.zeros(state.shape[1:], f32)
    for d in range(n_seq):
        ready[d] = running.astype(bf16)
        if d < n_seq - 1:
            running = carries[d] * running + landed[d].astype(f32)
    each(n_seq, lambda t: second(t).start())
    entering[mine] = ready[mine]

    def from_y(t):
        y = (at.y + at.ys - t) % at.ys

        def one(u):
            high, low = u % at.highs, u // at.highs
            seq = ((at.high + high) % at.highs) * at.lows + (at.low + low) % at.lows
            arrived((y * at.cores + at.core) * n_seq + seq)
            onward(y, seq, False, False)

        each(n_seq, one, 0)

    each(at.ys, from_y)
    each(n_seq, lambda t: second_in(t).wait_recv())

    def from_core(t):
        core = (at.core + t) % at.cores

        def one(k):
            arrived(((k // n_seq) * at.cores + core) * n_seq + k % n_seq)

        each(at.ys * n_seq, one, 0)

    each(at.cores, from_core)

    def sent(t):
        lead(t).wait_send()
        first(t).wait_send()
        second(t).wait_send()

    each(n_seq, sent)
    each(at.highs, lambda t: high_edge(t).wait_send())
    each(at.lows, lambda t: each(at.highs, lambda k: low_edge(t, k).wait_send(), 0))
    each(at.ys, lambda t: each(n_seq, lambda k: y_edge(t, k).wait_send(), 0))
    each(
        at.cores,
        lambda t: each(
            at.ys * n_seq, lambda k: core_edge(t, k // n_seq, k % n_seq).wait_send(), 0
        ),
    )


def scatter_kernel(
    n_dp, n_seq, grad, state, carries, pack, raw, sums, width, seg_c, x, proj, entering, carry,
    row_dot, col_dot, small, loss_part, rows, new_pack, new_rows, loss,
    part, leaving, by_core, by_y, by_low, by_high,
    staged, from_core, from_y, from_low, from_high, landed, ready,
    core_send, core_recv, y_send, y_recv, low_send, low_recv, high_send, high_recv,
    s_send, s_recv, r_send, r_recv, send, recv,
):
    at = Spot(n_dp, n_seq)
    at.meet(True)
    mine = at.seq
    back = lambda t: (mine + n_seq - t) % n_seq

    def first(t):
        p = (mine + t) % n_seq
        return remote(state.at[p], landed.at[mine], s_send.at[t], s_recv.at[t], at.seq_peer(t))

    def first_in(t):
        p = back(t)
        return remote(state.at[p], landed.at[p], s_send.at[t], s_recv.at[t], at.seq_peer(t))

    def second(t):
        p = (mine + t) % n_seq
        return remote(ready.at[p], leaving.at[mine], r_send.at[t], r_recv.at[t], at.seq_peer(t))

    def second_in(t):
        p = back(t)
        return remote(ready.at[p], leaving.at[p], r_send.at[t], r_recv.at[t], at.seq_peer(t))

    def core_edge(t, y, seq):
        core = (at.core + t) % at.cores
        k = (t * at.ys + y) * n_seq + seq
        return remote(
            grad.at[(y * at.cores + core) * n_seq + seq], from_core.at[k],
            core_send.at[k], core_recv.at[k], at.core_peer(t),
        )

    def y_edge(t, seq):
        k = t * n_seq + seq
        y = (at.y + t) % at.ys
        return remote(
            staged.at[y * n_seq + seq], from_y.at[k], y_send.at[k], y_recv.at[k], at.y_peer(t)
        )

    def low_edge(t, high):
        k = t * at.highs + high
        seq = high * at.lows + (at.low + t) % at.lows
        return remote(
            staged.at[at.y * n_seq + seq], from_low.at[k],
            low_send.at[k], low_recv.at[k], at.low_peer(t),
        )

    def high_edge(t):
        seq = ((at.high + t) % at.highs) * at.lows + at.low
        return remote(
            staged.at[at.y * n_seq + seq], from_high.at[t],
            high_send.at[t], high_recv.at[t], at.high_peer(t),
        )

    def chip_sum(y, seq):
        acc = grad[(y * at.cores + at.core) * n_seq + seq].astype(f32)
        for t in range(1, at.cores):
            core_edge(t, y, seq).wait_recv()
            acc = acc + from_core[(t * at.ys + y) * n_seq + seq].astype(f32)
        return acc

    def y_sum(seq):
        acc = chip_sum(at.y, seq)
        for t in range(1, at.ys):
            y_edge(t, seq).wait_recv()
            acc = acc + from_y[t * n_seq + seq].astype(f32)
        return acc

    def low_sum(high):
        acc = y_sum(high * at.lows + at.low)
        for t in range(1, at.lows):
            low_edge(t, high).wait_recv()
            acc = acc + from_low[t * at.highs + high].astype(f32)
        return acc

    def order(u):
        low = (at.low + 1 + u // at.highs) % at.lows
        return ((at.high + 1 + u) % at.highs) * at.lows + low

    each(n_seq, lambda t: first(t).start())

    def to_core(t):
        def one(k):
            core_edge(t, (at.y + 1 + k // n_seq) % at.ys, order(k % n_seq)).start()

        each(at.ys * n_seq, one, 0)

    each(at.cores, to_core)
    landed[mine] = state[mine]

    def to_y(t):
        y = (at.y + t) % at.ys

        def one(u):
            seq = order(u)
            staged[y * n_seq + seq] = chip_sum(y, seq).astype(bf16)
            y_edge(t, seq).start()

        each(n_seq, one, 0)

    each(at.ys, to_y)
    each(n_seq, lambda t: first_in(t).wait_recv())
    running = jnp.zeros(state.shape[1:], f32)
    for d in reversed(range(n_seq)):
        ready[d] = running.astype(bf16)
        if d > 0:
            running = carries[d] * running + landed[d].astype(f32)
    each(n_seq, lambda t: second(t).start())
    leaving[mine] = ready[mine]
    each(n_seq, lambda t: second_in(t).wait_recv())
    back_part(
        pack, raw, sums, width, seg_c, x, proj, leaving, entering, carry, row_dot, col_dot,
        small, loss_part, part,
    )

    def to_low(t):
        def one(u):
            high = (at.high + 1 + u) % at.highs
            seq = high * at.lows + (at.low + t) % at.lows
            staged[at.y * n_seq + seq] = y_sum(seq).astype(bf16)
            low_edge(t, high).start()

        each(at.highs, one, 0)

    each(at.lows, to_low)

    def to_high(t):
        high = (at.high + t) % at.highs
        staged[at.y * n_seq + high * at.lows + at.low] = low_sum(high).astype(bf16)
        high_edge(t).start()

    each(at.highs, to_high)
    acc = low_sum(at.high)
    for t in range(1, at.highs):
        high_edge(t).wait_recv()
        acc = acc + from_high[t].astype(f32)
    g = gain_rows(x.shape[1])
    square = jnp.sum(jnp.sum(acc * acc, axis=1, keepdims=True), axis=0, keepdims=True)
    place = lax.broadcasted_iota(jnp.int32, part.shape, 0)
    summed = jnp.where(place == g + 4, square, part[...])
    levels = [
        (by_core, at.cores, at.core, at.core_peer),
        (by_y, at.ys, at.y, at.y_peer),
        (by_low, at.lows, at.low, at.low_peer),
        (by_high, at.highs, at.high, at.high_peer),
    ]
    base = 0
    for held, count, digit, peer in levels:
        held[digit] = summed

        def edge(t, slot, held=held, digit=digit, peer=peer, base=base):
            return remote(held.at[digit], held.at[slot], send.at[base + t], recv.at[base + t], peer(t))

        each(count, lambda t: edge(t, digit).start())
        each(count, lambda t: edge(t, (digit + count - t) % count).wait_recv())
        summed = held[0]
        for k in range(1, count):
            summed = summed + held[k]
        each(count, lambda t: edge(t, digit).wait_send())
        base += count
    row = lax.broadcasted_iota(jnp.int32, summed.shape, 0)
    grads = jnp.where(row < g + 3, summed, 0.0)
    lane_sum = jnp.sum(grads * grads, axis=0, keepdims=True)
    norm_square = jnp.sum(lane_sum, axis=1, keepdims=True) + summed[g + 4 : g + 5, 0:1]
    factor = clip_limit / jnp.maximum(jnp.sqrt(norm_square), clip_limit)
    new_pack[...] = pack[...] - learn_rate * factor * grads
    new_rows[...] = rows[...] - learn_rate * factor * acc
    loss[...] = summed[g + 3 : g + 4, :]

    def sent(t):
        first(t).wait_send()
        second(t).wait_send()

    each(n_seq, sent)
    each(at.highs, lambda t: high_edge(t).wait_send())
    each(at.lows, lambda t: each(at.highs, lambda k: low_edge(t, k).wait_send(), 0))
    each(at.ys, lambda t: each(n_seq, lambda k: y_edge(t, k).wait_send(), 0))
    each(
        at.cores,
        lambda t: each(
            at.ys * n_seq, lambda k: core_edge(t, k // n_seq, k % n_seq).wait_send(), 0
        ),
    )


def call(body, outs, scratch=(), collective=None):
    extra = {}
    if collective is not None:
        extra = {"collective_id": collective, "has_side_effects": True}

    def run(*args):
        return pl.pallas_call(
            body,
            out_shape=tuple(jax.ShapeDtypeStruct(*o) for o in outs),
            in_specs=[SMEM if a.ndim == 1 else VMEM for a in args],
            out_specs=tuple([VMEM] * len(outs)),
            scratch_shapes=list(scratch),
            compiler_params=pltpu.CompilerParams(vmem_limit_bytes=LIMIT, **extra),
        )(*args)

    return run


def per_device(
    n_dp,
    n_seq,
    head_inputs,
    gate_inputs,
    state_proj,
    time_steps,
    token_ids,
    token_counts,
    teacher_out,
    out_weight,
    decay_log,
    step_bias,
    skip_gain,
    norm_gain,
):
    n = n_dp * n_seq
    x, z, target, raw = head_inputs[0], gate_inputs[0], teacher_out[0], time_steps[0]
    tokens, inner = x.shape
    ns = state_proj.shape[2] // 2
    heads = decay_log.shape[0]
    model = target.shape[1]
    share = out_weight.shape[0]
    piece = ns // n_seq
    g = gain_rows(inner)
    pack_rows = -(-(g + 5) // 8) * 8
    proj = state_proj[0]
    raw_t = raw.T
    ids_r = token_ids
    wide = lambda a: jnp.pad(a, (0, LANES - heads))[None]
    pack = jnp.concatenate(
        [
            norm_gain.reshape(g, LANES),
            wide(decay_log),
            wide(step_bias),
            wide(skip_gain),
            jnp.zeros((pack_rows - g - 3, LANES), f32),
        ]
    )
    rows = out_weight
    dma = pltpu.SemaphoreType.DMA
    losses = []
    per_head = ((tokens, heads), f32)
    for _ in range(STEPS):
        sums, sums_t, width, seg_c, seg_r, carry, full, entering, carries = call(
            functools.partial(gather_kernel, n_dp, n_seq),
            [
                per_head,
                ((heads, tokens), f32),
                per_head,
                ((tokens, 1), f32),
                ((1, tokens), f32),
                ((1, inner), f32),
                ((n, share, model), bf16),
                ((n_seq, piece, inner), bf16),
                ((n_seq, 1, inner), f32),
            ],
            [pltpu.VMEM((n_seq, piece, inner), bf16)] * 3
            + [
                dma((n,)),
                dma((n_seq,)),
                dma((n_seq * n_seq,)),
                dma((n,)),
                dma((n,)),
            ]
            + [dma((n_seq,))] * 6,
            0,
        )(pack, raw, raw_t, ids_r, x, proj, rows)
        weight = full.reshape(n * share, model)
        entering = entering.reshape(ns, inner)
        weight_grad, state_grad, row_dot, col_dot, small, loss = call(
            functools.partial(mix_kernel, n_dp),
            [
                ((inner, model), bf16),
                ((ns, inner), bf16),
                per_head,
                per_head,
                ((8, inner), f32),
                ((1, 1), f32),
            ],
            [
                pltpu.VMEM((tokens, inner), bf16),
                pltpu.VMEM((tokens, inner), f32),
                pltpu.VMEM((tokens, inner), bf16),
                pltpu.VMEM((tokens, inner), f32),
            ],
        )(
            token_counts, pack, sums, sums_t, width, seg_c, seg_r, x, z, proj, target, weight,
            entering,
        )
        pack, rows, loss_row = call(
            functools.partial(scatter_kernel, n_dp, n_seq),
            [((pack_rows, LANES), f32), ((share, model), f32), ((1, LANES), f32)],
            [pltpu.VMEM((pack_rows, LANES), f32), pltpu.VMEM((n_seq, piece, inner), bf16)]
            + [pltpu.VMEM((k, pack_rows, LANES), f32) for k in (n_dp, n_dp, n_seq, n_seq)]
            + [pltpu.VMEM((n, share, model), bf16)] * 3
            + [pltpu.VMEM((n_seq, share, model), bf16)] * 2
            + [pltpu.VMEM((n_seq, piece, inner), bf16)] * 2
            + [dma((n,))] * 4
            + [dma((n_seq,))] * 8
            + [dma((n,))] * 2,
            1,
        )(
            weight_grad.reshape(n, share, model),
            state_grad.reshape(n_seq, piece, inner),
            carries, pack, raw, sums, width, seg_c, x, proj, entering, carry, row_dot, col_dot,
            small, loss, rows,
        )
        losses.append(loss_row[0, 0])
    return (
        jnp.stack(losses),
        rows,
        pack[g, :heads],
        pack[g + 1, :heads],
        pack[g + 2, :heads],
        pack[:g].reshape(inner),
    )


def solution(mesh):
    in_specs = (
        P("dp", "seq", None),
        P("dp", "seq", None),
        P("dp", "seq", None),
        P("dp", "seq", None),
        P("dp", "seq"),
        P(),
        P("dp", "seq", None),
        P(("dp", "seq"), None),
        P(),
        P(),
        P(),
        P(),
    )
    out_specs = (P(), P(("dp", "seq"), None), P(), P(), P(), P())
    return jax.shard_map(
        functools.partial(per_device, mesh.shape["dp"], mesh.shape["seq"]),
        mesh=mesh,
        in_specs=in_specs,
        out_specs=out_specs,
        check_vma=False,
    )
```
